32 devices in a mesh: aa: 8 (over y, x, core), ba: 4 (over z).
Axes of the slice: x: 2, y: 2, z: 4, core: 2. Of those that a mesh axis runs over, the one named last changes fastest.
Arguments:
- images: float32 [32, 4, 128, 4096], P(('aa', 'ba')), may hold values from 0 to 0.06, as said below
- depth: int32 [32], replicated, may hold values from 0 to 31, as said below
- brick_map: int32 [32], replicated, may hold values from 0 to 31, as said below
Outputs:
- composite: float32 [4, 128, 4096], replicated
The draws below stay inside these ranges and needn't reach their ends.
Inputs may be any that keep to these rules, and one draw needn't show every extreme that they name: depth: a permutation of 0 to 31; the devices that share one index of ba hold bricks of 8 consecutive depth ranks. brick_map: a permutation of 0 to 31. images: channel 3 (alpha) lies between 0.002 and 0.06; channels 0 to 2 lie between 0 and the pixel's alpha.
All inputs are finite; a program needn't handle non-finite values.
Results may differ from the reference program's by a relative error of at most 0.00002.
Values sent between devices are 32-bit elements; how exact they have to be, the bound alone decides.
A program may use at most 128 MiB of HBM per device.

```python
import jax
import jax.numpy as jnp
from jax import lax

COLUMNS = 4096
ROWS = 128
N_AA = 8
N_BA = 4
DEVICES = 32


def order_tables(key):
    base = jax.random.fold_in(key, 7)
    key_group, key_inner, key_brick = jax.random.split(base, 3)
    group_slot = jax.random.permutation(key_group, N_BA).astype(jnp.int32)
    inner_keys = jax.random.split(key_inner, N_BA)
    inner = jax.vmap(lambda single: jax.random.permutation(single, N_AA))(inner_keys).astype(jnp.int32)
    device_rank = (group_slot[None, :] * N_AA + inner.T).reshape(DEVICES)
    brick_map = jax.random.permutation(key_brick, DEVICES).astype(jnp.int32)
    depth = jnp.zeros((DEVICES,), jnp.int32).at[brick_map].set(device_rank)
    return (depth, brick_map)


def draw_depth(key, part):
    return order_tables(key)[0]


def draw_brick_map(key, part):
    return order_tables(key)[1]


def draw_images(key, part):
    key_alpha, key_color = jax.random.split(jax.random.fold_in(key, 11), 2)
    shape = (DEVICES, 1, ROWS, COLUMNS)
    alpha = jnp.exp(jax.random.uniform(key_alpha, shape, jnp.float32, jnp.log(0.002), jnp.log(0.06)))
    color = alpha * jax.random.uniform(key_color, (DEVICES, 3, ROWS, COLUMNS), jnp.float32, 0.0, 1.0)
    return jnp.concatenate([color, alpha], axis=1).astype(jnp.float32)


def setup_inputs(seed: int = 0) -> dict:
    keys = jax.random.split(jax.random.key(seed), 4)
    images = draw_images(jax.random.fold_in(keys[3], 71), 0)
    depth = draw_depth(jax.random.fold_in(keys[3], 71), 0)
    brick_map = draw_brick_map(jax.random.fold_in(keys[3], 71), 0)
    return {"images": images, "depth": depth, "brick_map": brick_map}


def reference(images, depth, brick_map):
    device_rank = depth[brick_map].astype(jnp.int32)
    ordering = jnp.argsort(device_rank).astype(jnp.int32)

    def blend_step(total, index):
        piece = images[index]
        return total + (1.0 - total[3:4]) * piece, None

    start = jnp.zeros(images.shape[1:], jnp.float32)
    composite, unused = lax.scan(blend_step, start, ordering)
    return composite
```

```python
import functools

import jax
import jax.numpy as jnp
from jax import lax
from jax.experimental import pallas as pl
from jax.experimental.pallas import tpu as pltpu
from jax.sharding import PartitionSpec as P

MESH = pl.DeviceIdType.MESH
CHUNKS = 8
AHEAD = 2


def kernel(na, nb, nk, depth, brick, img, out, *scratch):
    recv = scratch[:nk]
    zsend = scratch[nk:2 * nk]
    zrecv = scratch[2 * nk:3 * nk]
    (full, order_a, order_b, own_sem, p_send, p_recv, z_send, z_recv,
     x_send, x_recv, g_send, g_recv, d_send, d_recv, out_sem) = scratch[3 * nk:]
    chips = na // 2
    width = recv[0].shape[3]
    wz = width // nb
    a = lax.axis_index("aa")
    b = lax.axis_index("ba")
    chip = a // 2
    core = a % 2
    sibling = chip * 2 + (1 - core)

    barrier = pltpu.get_barrier_semaphore()
    for j in range(1, na):
        pl.semaphore_signal(barrier, inc=1, device_id=(lax.rem(a + j, na), b), device_id_type=MESH)
    for j in range(1, nb):
        pl.semaphore_signal(barrier, inc=1, device_id=(a, lax.rem(b + j, nb)), device_id_type=MESH)
    pl.semaphore_wait(barrier, na + nb - 2)

    def own_copy(k):
        return pltpu.make_async_copy(img.at[:, a, :, pl.ds(k * width, width)], recv[k].at[a], own_sem.at[k])

    def p_copy(k, j, incoming=False):
        other = lax.rem(a + na - j, na) if incoming else lax.rem(a + j, na)
        slot = other if incoming else a
        return pltpu.make_async_remote_copy(
            src_ref=img.at[:, other, :, pl.ds(k * width, width)], dst_ref=recv[k].at[slot],
            send_sem=p_send.at[k, j], recv_sem=p_recv.at[k, j],
            device_id=(other, b), device_id_type=MESH)

    def z_copy(k, j, incoming=False):
        other = lax.rem(b + nb - j, nb) if incoming else lax.rem(b + j, nb)
        slot = other if incoming else b
        return pltpu.make_async_remote_copy(
            src_ref=zsend[k].at[other], dst_ref=zrecv[k].at[slot],
            send_sem=z_send.at[k, j], recv_sem=z_recv.at[k, j],
            device_id=(a, other), device_id_type=MESH)

    def x_copy(k, j, incoming=False):
        other = lax.rem(chip + chips - j, chips) if incoming else lax.rem(chip + j, chips)
        slot = other if incoming else chip
        piece = full.at[k, b, core, :, slot]
        return pltpu.make_async_remote_copy(
            src_ref=piece, dst_ref=piece, send_sem=x_send.at[k, j], recv_sem=x_recv.at[k, j],
            device_id=(other * 2 + core, b), device_id_type=MESH)

    def g_copy(k, j, incoming=False):
        other = lax.rem(b + nb - j, nb) if incoming else lax.rem(b + j, nb)
        slot = other if incoming else b
        piece = full.at[k, slot, core]
        return pltpu.make_async_remote_copy(
            src_ref=piece, dst_ref=piece, send_sem=g_send.at[k, j], recv_sem=g_recv.at[k, j],
            device_id=(a, other), device_id_type=MESH)

    def d_copy(k, j, incoming=False):
        slot = lax.rem(b + nb - j, nb)
        piece = full.at[k, slot, 1 - core if incoming else core]
        return pltpu.make_async_remote_copy(
            src_ref=piece, dst_ref=piece, send_sem=d_send.at[k, j], recv_sem=d_recv.at[k, j],
            device_id=(sibling, b), device_id_type=MESH)

    def out_copy(k, j, c):
        return pltpu.make_async_copy(
            full.at[k, j, c], out.at[:, :, c, :, pl.ds(k * width + j * wz, wz)], out_sem.at[k, j, c])

    def start_first(k):
        for j in range(1, na):
            p_copy(k, j).start()

    def blend(order, count, source, columns):
        total = None
        for position in range(count):
            slot = order[position]
            piece = [source[slot, c, :, columns] for c in range(4)]
            if total is None:
                total = piece
            else:
                left = 1.0 - total[3]
                total = [t + left * p for t, p in zip(total, piece)]
        return total

    for k in range(min(AHEAD, nk)):
        start_first(k)
    for k in range(nk):
        own_copy(k).start()

    ranks = [depth[brick[i * nb + b]] for i in range(na)]
    for position in range(na):
        picked = jnp.int32(0)
        for i in range(1, na):
            picked = jnp.where(lax.rem(ranks[i], na) == position, i, picked)
        order_a[position] = picked
    fronts = [depth[brick[j]] // na for j in range(nb)]
    for position in range(nb):
        picked = jnp.int32(0)
        for j in range(1, nb):
            picked = jnp.where(fronts[j] == position, j, picked)
        order_b[position] = picked

    for step in range(nk + 4):
        k = step
        if 0 <= k < nk:
            own_copy(k).wait()
            for j in range(1, na):
                p_copy(k, j, True).wait_recv()
            for j in range(nb):
                total = blend(order_a, na, recv[k], pl.ds(j * wz, wz))
                for c in range(4):
                    zsend[k][j, c] = total[c]
            for c in range(4):
                zrecv[k][b, c] = zsend[k][b, c]
            for j in range(1, nb):
                z_copy(k, j).start()
        k = step - 1
        if 0 <= k < nk:
            for j in range(1, nb):
                z_copy(k, j, True).wait_recv()
            total = blend(order_b, nb, zrecv[k], pl.ds(0, wz))
            for c in range(4):
                full[k, b, core, c, chip] = total[c]
            for j in range(1, chips):
                x_copy(k, j).start()
        k = step + AHEAD
        if k < nk:
            start_first(k)
        k = step - 2
        if 0 <= k < nk:
            for j in range(1, chips):
                x_copy(k, j, True).wait_recv()
            for j in range(1, nb):
                g_copy(k, j).start()
            d_copy(k, 0).start()
        k = step - 3
        if 0 <= k < nk:
            for j in range(1, nb):
                g_copy(k, j, True).wait_recv()
                d_copy(k, j).start()
        k = step - 4
        if 0 <= k < nk:
            for j in range(nb):
                d_copy(k, j, True).wait_recv()
            for j in range(nb):
                for c in range(2):
                    out_copy(k, j, c).start()
    for k in range(nk):
        for j in range(1, na):
            p_copy(k, j).wait_send()
        for j in range(1, nb):
            z_copy(k, j).wait_send()
            g_copy(k, j).wait_send()
        for j in range(1, chips):
            x_copy(k, j).wait_send()
        for j in range(nb):
            d_copy(k, j).wait_send()
            for c in range(2):
                out_copy(k, j, c).wait()


def local(images, depth, brick_map):
    na = lax.axis_size("aa")
    nb = lax.axis_size("ba")
    rows, columns = images.shape[2], images.shape[3]
    band = rows // na
    nk = min(CHUNKS, columns // (128 * nb))
    width = columns // nk
    wz = width // nb
    chips = na // 2
    dma = pltpu.SemaphoreType.DMA
    f32 = jnp.float32
    scratch = [pltpu.VMEM((na, 4, band, width), f32) for _ in range(nk)]
    scratch += [pltpu.VMEM((nb, 4, band, wz), f32) for _ in range(2 * nk)]
    scratch += [
        pltpu.VMEM((nk, nb, 2, 4, chips, band, wz), f32),
        pltpu.SMEM((na,), jnp.int32), pltpu.SMEM((nb,), jnp.int32),
        dma((nk,)), dma((nk, na)), dma((nk, na)), dma((nk, nb)), dma((nk, nb)),
        dma((nk, chips)), dma((nk, chips)), dma((nk, nb)), dma((nk, nb)),
        dma((nk, nb)), dma((nk, nb)), dma((nk, nb, 2)),
    ]
    smem = pl.BlockSpec(memory_space=pltpu.SMEM)
    hbm = pl.BlockSpec(memory_space=pltpu.MemorySpace.HBM)
    composite = pl.pallas_call(
        functools.partial(kernel, na, nb, nk),
        out_shape=jax.ShapeDtypeStruct((4, chips, 2, band, columns), f32),
        in_specs=[smem, smem, hbm],
        out_specs=hbm,
        scratch_shapes=scratch,
        compiler_params=pltpu.CompilerParams(
            collective_id=0, has_side_effects=True, vmem_limit_bytes=48 * 1024 * 1024),
    )(depth, brick_map, images.reshape(4, na, band, columns))
    return composite.reshape(4, rows, columns)


def solution(mesh):
    placed = (P(("aa", "ba"), None, None, None), P(), P())
    return jax.shard_map(local, mesh=mesh, in_specs=placed, out_specs=P(), check_vma=False)
```

```python
import functools

import jax
import jax.numpy as jnp
from jax import lax
from jax.experimental import pallas as pl
from jax.experimental.pallas import tpu as pltpu
from jax.sharding import PartitionSpec as P

MESH = pl.DeviceIdType.MESH
CHUNKS = 8
AHEAD = 2
COLUMN_FIRST = 4


def kernel(na, nb, nk, depth, brick, img, out, *scratch):
    recv = scratch[:nk]
    zsend = scratch[nk:2 * nk]
    zrecv = scratch[2 * nk:3 * nk]
    (full, order_a, order_b, own_sem, p_send, p_recv, z_send, z_recv,
     x_send, x_recv, g_send, g_recv, d_send, d_recv, out_sem) = scratch[3 * nk:]
    chips = na // 2
    column_first = range(nk - min(COLUMN_FIRST, nk), nk)
    strips = [nb if k in column_first else chips for k in range(nk)]
    blocks = [chips if k in column_first else nb for k in range(nk)]
    width = recv[0].shape[3]
    wz = width // nb
    a = lax.axis_index("aa")
    b = lax.axis_index("ba")
    chip = a // 2
    core = a % 2
    sibling = chip * 2 + (1 - core)

    barrier = pltpu.get_barrier_semaphore()
    for j in range(1, na):
        pl.semaphore_signal(barrier, inc=1, device_id=(lax.rem(a + j, na), b), device_id_type=MESH)
    for j in range(1, nb):
        pl.semaphore_signal(barrier, inc=1, device_id=(a, lax.rem(b + j, nb)), device_id_type=MESH)
    pl.semaphore_wait(barrier, na + nb - 2)

    def own_copy(k):
        return pltpu.make_async_copy(img.at[:, a, :, pl.ds(k * width, width)], recv[k].at[a], own_sem.at[k])

    def p_copy(k, j, incoming=False):
        other = lax.rem(a + na - j, na) if incoming else lax.rem(a + j, na)
        slot = other if incoming else a
        return pltpu.make_async_remote_copy(
            src_ref=img.at[:, other, :, pl.ds(k * width, width)], dst_ref=recv[k].at[slot],
            send_sem=p_send.at[k, j], recv_sem=p_recv.at[k, j],
            device_id=(other, b), device_id_type=MESH)

    def z_copy(k, j, incoming=False):
        other = lax.rem(b + nb - j, nb) if incoming else lax.rem(b + j, nb)
        slot = other if incoming else b
        return pltpu.make_async_remote_copy(
            src_ref=zsend[k].at[other], dst_ref=zrecv[k].at[slot],
            send_sem=z_send.at[k, j], recv_sem=z_recv.at[k, j],
            device_id=(a, other), device_id_type=MESH)

    def peer_chip(j, incoming):
        return lax.rem(chip + chips - j, chips) if incoming else lax.rem(chip + j, chips)

    def peer_row(j, incoming):
        return lax.rem(b + nb - j, nb) if incoming else lax.rem(b + j, nb)

    def strip_copy(k, j, incoming=False):
        if k in column_first:
            other = peer_row(j, incoming)
            piece = full.at[k, other if incoming else b, core, :, chip]
            target = (a, other)
        else:
            other = peer_chip(j, incoming)
            piece = full.at[k, b, core, :, other if incoming else chip]
            target = (other * 2 + core, b)
        return pltpu.make_async_remote_copy(
            src_ref=piece, dst_ref=piece, send_sem=x_send.at[k, j], recv_sem=x_recv.at[k, j],
            device_id=target, device_id_type=MESH)

    def block(k, slot, side):
        return full.at[k, :, side, :, slot] if k in column_first else full.at[k, slot, side]

    def block_copy(k, j, incoming=False):
        if k in column_first:
            other = peer_chip(j, incoming)
            target, mine = (other * 2 + core, b), chip
        else:
            other = peer_row(j, incoming)
            target, mine = (a, other), b
        piece = block(k, other if incoming else mine, core)
        return pltpu.make_async_remote_copy(
            src_ref=piece, dst_ref=piece, send_sem=g_send.at[k, j], recv_sem=g_recv.at[k, j],
            device_id=target, device_id_type=MESH)

    def d_copy(k, j, incoming=False):
        slot = peer_chip(j, True) if k in column_first else peer_row(j, True)
        piece = block(k, slot, 1 - core if incoming else core)
        return pltpu.make_async_remote_copy(
            src_ref=piece, dst_ref=piece, send_sem=d_send.at[k, j], recv_sem=d_recv.at[k, j],
            device_id=(sibling, b), device_id_type=MESH)

    def out_copy(k, j, c):
        return pltpu.make_async_copy(
            full.at[k, j, c], out.at[:, :, c, :, pl.ds(k * width + j * wz, wz)], out_sem.at[k, j, c])

    def start_first(k):
        for j in range(1, na):
            p_copy(k, j).start()

    def blend(order, count, source, columns):
        total = None
        for position in range(count):
            slot = order[position]
            piece = [source[slot, c, :, columns] for c in range(4)]
            if total is None:
                total = piece
            else:
                left = 1.0 - total[3]
                total = [t + left * p for t, p in zip(total, piece)]
        return total

    for k in range(min(AHEAD, nk)):
        start_first(k)
    for k in range(nk):
        own_copy(k).start()

    ranks = [depth[brick[i * nb + b]] for i in range(na)]
    for position in range(na):
        picked = jnp.int32(0)
        for i in range(1, na):
            picked = jnp.where(lax.rem(ranks[i], na) == position, i, picked)
        order_a[position] = picked
    fronts = [depth[brick[j]] // na for j in range(nb)]
    for position in range(nb):
        picked = jnp.int32(0)
        for j in range(1, nb):
            picked = jnp.where(fronts[j] == position, j, picked)
        order_b[position] = picked

    for step in range(nk + 4):
        k = step
        if 0 <= k < nk:
            own_copy(k).wait()
            for j in range(1, na):
                p_copy(k, j, True).wait_recv()
            for j in range(nb):
                total = blend(order_a, na, recv[k], pl.ds(j * wz, wz))
                for c in range(4):
                    zsend[k][j, c] = total[c]
            for c in range(4):
                zrecv[k][b, c] = zsend[k][b, c]
            for j in range(1, nb):
                z_copy(k, j).start()
        k = step - 1
        if 0 <= k < nk:
            for j in range(1, nb):
                z_copy(k, j, True).wait_recv()
            total = blend(order_b, nb, zrecv[k], pl.ds(0, wz))
            for c in range(4):
                full[k, b, core, c, chip] = total[c]
            for j in range(1, strips[k]):
                strip_copy(k, j).start()
        k = step + AHEAD
        if k < nk:
            start_first(k)
        k = step - 2
        if 0 <= k < nk:
            for j in range(1, strips[k]):
                strip_copy(k, j, True).wait_recv()
            for j in range(1, blocks[k]):
                block_copy(k, j).start()
            d_copy(k, 0).start()
        k = step - 3
        if 0 <= k < nk:
            for j in range(1, blocks[k]):
                block_copy(k, j, True).wait_recv()
                d_copy(k, j).start()
        k = step - 4
        if 0 <= k < nk:
            for j in range(blocks[k]):
                d_copy(k, j, True).wait_recv()
            for j in range(nb):
                for c in range(2):
                    out_copy(k, j, c).start()
    for k in range(nk):
        for j in range(1, na):
            p_copy(k, j).wait_send()
        for j in range(1, nb):
            z_copy(k, j).wait_send()
        for j in range(1, strips[k]):
            strip_copy(k, j).wait_send()
        for j in range(1, blocks[k]):
            block_copy(k, j).wait_send()
        for j in range(blocks[k]):
            d_copy(k, j).wait_send()
        for j in range(nb):
            for c in range(2):
                out_copy(k, j, c).wait()


def local(images, depth, brick_map):
    na = lax.axis_size("aa")
    nb = lax.axis_size("ba")
    rows, columns = images.shape[2], images.shape[3]
    band = rows // na
    nk = min(CHUNKS, columns // (128 * nb))
    width = columns // nk
    wz = width // nb
    chips = na // 2
    most = max(chips, nb)
    dma = pltpu.SemaphoreType.DMA
    f32 = jnp.float32
    scratch = [pltpu.VMEM((na, 4, band, width), f32) for _ in range(nk)]
    scratch += [pltpu.VMEM((nb, 4, band, wz), f32) for _ in range(2 * nk)]
    scratch += [
        pltpu.VMEM((nk, nb, 2, 4, chips, band, wz), f32),
        pltpu.SMEM((na,), jnp.int32), pltpu.SMEM((nb,), jnp.int32),
        dma((nk,)), dma((nk, na)), dma((nk, na)), dma((nk, nb)), dma((nk, nb)),
        dma((nk, most)), dma((nk, most)), dma((nk, most)), dma((nk, most)),
        dma((nk, most)), dma((nk, most)), dma((nk, nb, 2)),
    ]
    smem = pl.BlockSpec(memory_space=pltpu.SMEM)
    hbm = pl.BlockSpec(memory_space=pltpu.MemorySpace.HBM)
    composite = pl.pallas_call(
        functools.partial(kernel, na, nb, nk),
        out_shape=jax.ShapeDtypeStruct((4, chips, 2, band, columns), f32),
        in_specs=[smem, smem, hbm],
        out_specs=hbm,
        scratch_shapes=scratch,
        compiler_params=pltpu.CompilerParams(
            collective_id=0, has_side_effects=True, vmem_limit_bytes=48 * 1024 * 1024),
    )(depth, brick_map, images.reshape(4, na, band, columns))
    return composite.reshape(4, rows, columns)


def solution(mesh):
    placed = (P(("aa", "ba"), None, None, None), P(), P())
    return jax.shard_map(local, mesh=mesh, in_specs=placed, out_specs=P(), check_vma=False)
```
